8 devices in a mesh: batch: 1 (over z), cx: 2 (over y), cy: 4 (over x, core).
Axes of the slice: x: 2, y: 2, z: 1, core: 2. Of those that a mesh axis runs over, the one named last changes fastest.
Arguments:
- q_tok: bfloat16 [1024, 40, 128], P(('batch', 'cx', 'cy'))
- k_tok: bfloat16 [1024, 8, 128], P(('batch', 'cx', 'cy'))
- v_tok: bfloat16 [1024, 8, 128], P(('batch', 'cx', 'cy'))
Outputs:
- output: bfloat16 [1024, 40, 128], P(('batch', 'cx', 'cy'))
All inputs are finite; a program needn't handle non-finite values.
Results may differ from the reference program's by a relative error of at most 0.00437211.
Values are sent between devices in bfloat16 or wider.
A program may use at most 1 GiB of HBM per device.

```python
import jax
import jax.numpy as jnp
from jax import lax

HEADS = 40
KV_HEADS = 8
HEAD = 128
TOKENS_DEV = 128
RANKS = 8
SEQ = TOKENS_DEV * RANKS
GROUP = HEADS // KV_HEADS
Q_SCALE = HEAD ** -0.5


def setup_inputs(seed: int = 0, part: int = 0) -> dict:
    base_key = jax.random.fold_in(jax.random.key(seed), part)
    key_q, key_k, key_v = jax.random.split(base_key, 3)
    q_tok = jax.random.normal(key_q, (SEQ, HEADS, HEAD), jnp.float32)
    k_tok = jax.random.normal(key_k, (SEQ, KV_HEADS, HEAD), jnp.float32)
    v_tok = jax.random.normal(key_v, (SEQ, KV_HEADS, HEAD), jnp.float32)
    return {"q_tok": q_tok.astype(jnp.bfloat16), "k_tok": k_tok.astype(jnp.bfloat16), "v_tok": v_tok.astype(jnp.bfloat16)}


def reference(q_tok, k_tok, v_tok):
    q_blocks = q_tok.reshape(RANKS, TOKENS_DEV, KV_HEADS, GROUP, HEAD)
    k_blocks = k_tok.reshape(RANKS, TOKENS_DEV, KV_HEADS, HEAD)
    v_blocks = v_tok.reshape(RANKS, TOKENS_DEV, KV_HEADS, HEAD)
    positions = jnp.arange(TOKENS_DEV)
    diag_keep = positions[:, None, None] >= positions[None, None, :]
    stat_shape = (KV_HEADS, TOKENS_DEV, GROUP)

    def query_block(q_item):
        q_idx, q_blk = q_item
        q_f32 = q_blk.astype(jnp.float32)

        def key_step(running, kv_item):
            k_idx, k_blk, v_blk = kv_item

            def visit(state):
                run_max, run_sum, out_acc = state
                scores = jnp.einsum("qgnd,kgd->gqnk", q_f32, k_blk.astype(jnp.float32)) * Q_SCALE
                keep_mask = jnp.logical_or(k_idx < q_idx, diag_keep)
                scores = jnp.where(keep_mask, scores, -jnp.inf)
                new_max = jnp.maximum(run_max, jnp.max(scores, axis=-1))
                p_blk = jnp.exp(scores - new_max[..., None])
                rescale = jnp.exp(run_max - new_max)
                new_sum = run_sum * rescale + jnp.sum(p_blk, axis=-1)
                p_low = p_blk.astype(jnp.bfloat16).astype(jnp.float32)
                new_acc = out_acc * rescale[..., None] + jnp.einsum("gqnk,kgd->gqnd", p_low, v_blk.astype(jnp.float32))
                return new_max, new_sum, new_acc

            def skip_block(state):
                return state

            return lax.cond(k_idx <= q_idx, visit, skip_block, running), None

        initial = (jnp.full(stat_shape, -jnp.inf, jnp.float32), jnp.zeros(stat_shape, jnp.float32), jnp.zeros(stat_shape + (HEAD,), jnp.float32))
        final_state, _ = lax.scan(key_step, initial, (jnp.arange(RANKS), k_blocks, v_blocks))
        run_max, run_sum, out_acc = final_state
        out_blk = (out_acc / run_sum[..., None]).astype(jnp.bfloat16)
        return jnp.transpose(out_blk, (1, 0, 2, 3)).reshape(TOKENS_DEV, HEADS, HEAD)

    out_blocks = lax.map(query_block, (jnp.arange(RANKS), q_blocks))
    return out_blocks.reshape(SEQ, HEADS, HEAD)
```

```python
import functools
import math

import jax
import jax.numpy as jnp
from jax import lax
from jax.experimental import pallas as pl
from jax.experimental.pallas import tpu as pltpu
from jax.sharding import PartitionSpec as P

MESH = pl.DeviceIdType.MESH
F32 = jnp.float32
BF16 = jnp.bfloat16

K_UNITS = ((0, 4, 0), (4, 4, 1))
V_UNITS = tuple((h, 1, h % 2) for h in range(8))
NK, NV = len(K_UNITS), len(V_UNITS)
NU = NK + NV
X, Y, Z, PT, PX, PY, PZ = range(7)
OWN = 3


def kernel(q_hbm, k_hbm, v_hbm, o_ref, kbuf, vbuf, qt, s_buf, p_buf, mp, linv, q_raw, k_raw, v_raw, f_buf, o32, lsem, ssem, rsem):
    tokens, num_heads, dim = q_hbm.shape
    num_kv = k_hbm.shape[1]
    group = num_heads // num_kv
    rows = group * tokens
    pair = 2 * tokens
    iy, cy = lax.axis_index("cx"), lax.axis_index("cy")
    ix, core = cy // 2, cy % 2
    cy_x = (cy + 2) % 4
    cy_p = cy + 1 - 2 * core
    cy_xp = (cy_p + 2) % 4
    iy_o = 1 - iy
    rank_of = {OWN + 10: iy * 4 + cy, X: iy * 4 + cy_x, Y: iy_o * 4 + cy, Z: iy_o * 4 + cy_x, PT: iy * 4 + cy_p, PX: iy * 4 + cy_xp, PY: iy_o * 4 + cy_p, PZ: iy_o * 4 + cy_xp}
    ME = OWN + 10
    dev_x, dev_y, dev_p = (0, iy, cy_x), (0, iy_o, cy), (0, iy, cy_p)
    chip_of = {X: iy * 2 + 1 - ix, Y: iy_o * 2 + ix, Z: iy_o * 2 + 1 - ix, OWN: iy * 2 + ix}

    loads = [pltpu.make_async_copy(k_hbm, k_raw, lsem.at[0]), pltpu.make_async_copy(v_hbm, v_raw, lsem.at[1]), pltpu.make_async_copy(q_hbm, q_raw, lsem.at[2])]
    for load in loads:
        load.start()
    barrier = pltpu.get_barrier_semaphore()
    for dev in (dev_x, dev_y, dev_p):
        pl.semaphore_signal(barrier, inc=1, device_id=dev, device_id_type=MESH)

    def split_heads(raw, heads, put):
        step = 32

        def widen(i, carry):
            t = pl.multiple_of(i * step, step)
            f_buf[pl.ds(pl.multiple_of(t * heads, step * heads), step * heads), :] = raw[pl.ds(t, step)].astype(F32).reshape(step * heads, dim)
            return carry

        lax.fori_loop(0, tokens // step, widen, 0)
        for h in range(heads):
            put(h, f_buf[pl.ds(h, tokens, stride=heads), :].astype(BF16))

    my_rows = pl.ds(pl.multiple_of(rank_of[ME] * tokens, tokens), tokens)

    def put_k(h, val):
        kbuf[h, my_rows, :] = val

    def put_v(h, val):
        vbuf[h, my_rows, :] = val

    def put_q(h, val):
        qt[h // group, pl.ds((h % group) * tokens, tokens), :] = val

    loads[0].wait()
    split_heads(k_raw, num_kv, put_k)
    loads[1].wait()
    split_heads(v_raw, num_kv, put_v)
    pl.semaphore_wait(barrier, 3)

    sends = []

    def piece(unit, src):
        buf, (h0, n, _) = (kbuf, K_UNITS[unit]) if unit < NK else (vbuf, V_UNITS[unit - NK])
        return buf.at[pl.ds(h0, n), pl.ds(pl.multiple_of(rank_of[src] * tokens, tokens), tokens), :]

    def send(unit, src, dev, as_src):
        ref = piece(unit, src)
        copy = pltpu.make_async_remote_copy(ref, ref, ssem.at[len(sends)], rsem.at[as_src * NU + unit], device_id=dev, device_id_type=MESH)
        copy.start()
        sends.append(copy)

    def arrive(unit, src):
        ref = piece(unit, src)
        pltpu.make_async_remote_copy(ref, ref, ssem.at[0], rsem.at[src * NU + unit], device_id=dev_p, device_id_type=MESH).wait_recv()

    def path(unit):
        return (K_UNITS + V_UNITS)[unit][2]

    def own_link(unit, which):
        send(unit, ME, (dev_x, dev_y)[which], (X, Y)[which])

    def take(unit, src, relay=True):
        arrive(unit, src)
        if src == X and path(unit) == 0 and relay:
            send(unit, X, dev_y, Z)
        if src == Y and path(unit) == 1 and relay:
            send(unit, Y, dev_x, Z)
        send(unit, src, dev_p, {X: PX, Y: PY, Z: PZ}[src])

    own_link(0, 0)
    own_link(1, 1)
    own_link(1, 0)
    own_link(0, 1)
    for u in range(NU):
        send(u, ME, dev_p, PT)

    loads[2].wait()
    split_heads(q_raw, num_heads, put_q)

    def scores(blk, h):
        kk = kbuf[h, pl.ds(pl.multiple_of(chip_of[blk] * pair, pair), pair), :]
        return lax.dot_general(qt[h], kk, (((1,), (1,)), ((), ())), preferred_element_type=F32)

    def score_own(h):
        s = scores(OWN, h)
        q_pos = lax.broadcasted_iota(jnp.int32, (rows, pair), 0) % tokens + core * tokens
        k_pos = lax.broadcasted_iota(jnp.int32, (rows, pair), 1)
        s = jnp.where(k_pos <= q_pos, s, -jnp.inf)
        s_buf[OWN, h] = s
        mp[h] = jnp.maximum(s[:, :tokens], s[:, tokens:])

    def score_other(blk, h):
        s = scores(blk, h)
        s_buf[blk, h] = s
        mp[h] = jnp.maximum(mp[h], jnp.maximum(s[:, :tokens], s[:, tokens:]))

    def for_heads(h0, n, body):
        def step(h, carry):
            body(h)
            return carry

        lax.fori_loop(h0, h0 + n, step, 0)

    needed = {X: ix == 1, Y: iy == 1, Z: iy == 1}

    def scores_of(blk, unit):
        h0, n, _ = K_UNITS[unit]
        arrive(unit, {X: PX, Y: PY, Z: PZ}[blk])

        @pl.when(needed[blk])
        def _():
            for_heads(h0, n, functools.partial(score_other, blk))

    for u in range(NK):
        arrive(u, PT)
    for_heads(0, num_kv, score_own)

    take(0, X)
    take(1, Y)
    for v in (0, 1):
        own_link(NK + v, 0)
        own_link(NK + v, 1)
    scores_of(X, 0)
    scores_of(Y, 1)
    take(1, X)
    take(0, Y)
    scores_of(X, 1)
    scores_of(Y, 0)
    take(0, Z)
    take(1, Z)
    scores_of(Z, 0)
    scores_of(Z, 1)

    log2_scale = dim ** -0.5 * math.log2(math.e)
    step_rows = 64

    def probs(h):
        def chunk(i, carry):
            r = pl.ds(pl.multiple_of(i * step_rows, step_rows), step_rows)
            m = jnp.max(mp[h, r, :], axis=-1, keepdims=True) * log2_scale
            total = jnp.zeros((step_rows, tokens), F32)

            def one(blk, total):
                p = jnp.exp2(s_buf[blk, h, r, :] * log2_scale - m)
                p_buf[blk, h, r, :] = p.astype(BF16)
                return total + (p[:, :tokens] + p[:, tokens:])

            total = one(OWN, total)
            for blk in (X, Y, Z):
                def none(blk, total):
                    p_buf[blk, h, r, :] = jnp.zeros((step_rows, pair), BF16)
                    return total

                total = lax.cond(needed[blk], functools.partial(one, blk), functools.partial(none, blk), total)
            linv[h, r, :] = 1.0 / jnp.broadcast_to(jnp.sum(total, axis=-1, keepdims=True), (step_rows, dim))
            return carry

        lax.fori_loop(0, rows // step_rows, chunk, 0)

    def outputs(h):
        acc = None
        for blk in (OWN, X, Y, Z):
            vv = vbuf[h, pl.ds(pl.multiple_of(chip_of[blk] * pair, pair), pair), :]
            part = lax.dot_general(p_buf[blk, h], vv, (((1,), (0,)), ((), ())), preferred_element_type=F32)
            acc = part if acc is None else acc + part
        out = acc * linv[h]
        for n in range(group):
            o32[pl.ds(h * group + n, tokens, stride=num_heads), :] = out[n * tokens : (n + 1) * tokens, :]

    def finish(v):
        for src in (PT, PX, PY, PZ):
            arrive(NK + v, src)
        h0, n, _ = V_UNITS[v]
        for h in range(h0, h0 + n):
            outputs(h)

    for v in range(NV):
        take(NK + v, X)
        take(NK + v, Y)
        if v + 2 < NV:
            own_link(NK + v + 2, 0)
            own_link(NK + v + 2, 1)
        if v >= 2:
            take(NK + v - 2, Z)
        h0, n, _ = V_UNITS[v]
        for_heads(h0, n, probs)
        if v >= 3:
            finish(v - 3)
    take(NK + NV - 2, Z)
    finish(NV - 3)
    take(NK + NV - 1, Z)
    finish(NV - 2)
    finish(NV - 1)

    def narrow(i, carry):
        t = pl.multiple_of(i * 16, 16)
        o_ref[pl.ds(t, 16)] = o32[pl.ds(pl.multiple_of(t * num_heads, 16 * num_heads), 16 * num_heads), :].reshape(16, num_heads, dim).astype(BF16)
        return carry

    lax.fori_loop(0, tokens // 16, narrow, 0)
    for copy in sends:
        copy.wait_send()


def solution(mesh):
    seq_spec = P(("batch", "cx", "cy"), None, None)
    ranks = mesh.shape["cx"] * mesh.shape["cy"]

    def local(q, k, v):
        tokens, heads, dim = q.shape
        kv = k.shape[1]
        rows = heads // kv * tokens
        n_sends = 3 * NU + NU + 3 * NU
        hbm = pl.BlockSpec(memory_space=pltpu.HBM)
        return pl.pallas_call(
            kernel,
            out_shape=jax.ShapeDtypeStruct(q.shape, q.dtype),
            in_specs=[hbm, hbm, hbm],
            out_specs=pl.BlockSpec(memory_space=pltpu.VMEM),
            scratch_shapes=[
                pltpu.VMEM((kv, ranks * tokens, dim), BF16),
                pltpu.VMEM((kv, ranks * tokens, dim), BF16),
                pltpu.VMEM((kv, rows, dim), BF16),
                pltpu.VMEM((4, kv, rows, 2 * tokens), F32),
                pltpu.VMEM((4, kv, rows, 2 * tokens), BF16),
                pltpu.VMEM((kv, rows, dim), F32),
                pltpu.VMEM((kv, rows, dim), F32),
                pltpu.VMEM((tokens, heads, dim), BF16),
                pltpu.VMEM((tokens, kv, dim), BF16),
                pltpu.VMEM((tokens, kv, dim), BF16),
                pltpu.VMEM((tokens * heads, dim), F32),
                pltpu.VMEM((tokens * heads, dim), F32),
                pltpu.SemaphoreType.DMA((3,)),
                pltpu.SemaphoreType.DMA((n_sends,)),
                pltpu.SemaphoreType.DMA((7 * NU,)),
            ],
            compiler_params=pltpu.CompilerParams(collective_id=0, has_side_effects=True, vmem_limit_bytes=56 * 2**20),
        )(q, k, v)

    return jax.shard_map(local, mesh=mesh, in_specs=(seq_spec, seq_spec, seq_spec), out_specs=seq_spec, check_vma=False)
```

```python
import math

import jax
import jax.numpy as jnp
from jax import lax
from jax.experimental import pallas as pl
from jax.experimental.pallas import tpu as pltpu
from jax.sharding import PartitionSpec as P

MESH = pl.DeviceIdType.MESH
F32 = jnp.float32
BF16 = jnp.bfloat16

K_UNITS = ((0, 4, 0), (4, 4, 1))
V_UNITS = ((0, 2, 0), (2, 2, 1), (4, 2, 0), (6, 2, 1))
W_UNITS = tuple((h, 1, (h // 2) % 2) for h in range(8))
NK, NV, NW = len(K_UNITS), len(V_UNITS), len(W_UNITS)
UNITS = K_UNITS + V_UNITS + W_UNITS
NU = len(UNITS)
X, Y, Z, OWN = range(4)
PT, PX, PY, PZ = 3, 4, 5, 6
ME = 7
ROLE_BLOCKS = ((OWN,), (OWN, X), (OWN, Y, Z), (OWN, X, Y, Z))


def kernel(q_hbm, k_hbm, v_hbm, o_ref, kbuf, vbuf, qt, s_buf, p_buf, mp, lsum, acc, q_raw, k_raw, v_raw, f_buf, lsem, ssem, rsem):
    tokens, num_heads, dim = q_hbm.shape
    num_kv = k_hbm.shape[1]
    group = num_heads // num_kv
    rows = group * tokens
    pair = 2 * tokens
    iy, cy = lax.axis_index("cx"), lax.axis_index("cy")
    ix, core = cy // 2, cy % 2
    chip = iy * 2 + ix
    cy_x = (cy + 2) % 4
    cy_p = cy + 1 - 2 * core
    cy_xp = (cy_p + 2) % 4
    iy_o = 1 - iy
    rank_of = {ME: iy * 4 + cy, X: iy * 4 + cy_x, Y: iy_o * 4 + cy, Z: iy_o * 4 + cy_x, PT: iy * 4 + cy_p, PX: iy * 4 + cy_xp, PY: iy_o * 4 + cy_p, PZ: iy_o * 4 + cy_xp}
    dev_x, dev_y, dev_p = (0, iy, cy_x), (0, iy_o, cy), (0, iy, cy_p)
    chip_of = {X: iy * 2 + 1 - ix, Y: iy_o * 2 + ix, Z: iy_o * 2 + 1 - ix, OWN: chip}

    loads = [pltpu.make_async_copy(k_hbm, k_raw, lsem.at[0]), pltpu.make_async_copy(v_hbm, v_raw, lsem.at[1]), pltpu.make_async_copy(q_hbm, q_raw, lsem.at[2])]
    for load in loads:
        load.start()
    barrier = pltpu.get_barrier_semaphore()
    for dev in (dev_x, dev_y, dev_p):
        pl.semaphore_signal(barrier, inc=1, device_id=dev, device_id_type=MESH)

    def split_heads(raw, heads, put):
        step = 32

        def widen(i, carry):
            t = pl.multiple_of(i * step, step)
            f_buf[pl.ds(pl.multiple_of(t * heads, step * heads), step * heads), :] = raw[pl.ds(t, step)].astype(F32).reshape(step * heads, dim)
            return carry

        lax.fori_loop(0, tokens // step, widen, 0)
        for h in range(heads):
            put(h, f_buf[pl.ds(h, tokens, stride=heads), :].astype(BF16))

    my_rows = pl.ds(pl.multiple_of(rank_of[ME] * tokens, tokens), tokens)

    def put_k(h, val):
        kbuf[h, my_rows, :] = val

    def put_v(h, val):
        vbuf[h, my_rows, :] = val

    def put_q(h, val):
        qt[h // group, pl.ds((h % group) * tokens, tokens), :] = val

    sends = []

    def piece(unit, src):
        h0, n, _ = UNITS[unit]
        buf = kbuf if unit < NK else vbuf
        return buf.at[pl.ds(h0, n), pl.ds(pl.multiple_of(rank_of[src] * tokens, tokens), tokens), :]

    def send(unit, src, dev, as_src):
        ref = piece(unit, src)
        copy = pltpu.make_async_remote_copy(ref, ref, ssem.at[len(sends)], rsem.at[as_src * NU + unit], device_id=dev, device_id_type=MESH)
        copy.start()
        sends.append(copy)

    def arrive(unit, src):
        ref = piece(unit, src)
        pltpu.make_async_remote_copy(ref, ref, ssem.at[0], rsem.at[src * NU + unit], device_id=dev_p, device_id_type=MESH).wait_recv()

    def own_link(unit, which):
        send(unit, ME, (dev_x, dev_y)[which], (X, Y)[which])

    def share(unit, src):
        send(unit, src, dev_p, {X: PX, Y: PY, Z: PZ}[src])

    def relay(unit, src):
        send(unit, src, {X: dev_y, Y: dev_x}[src], Z)

    def by_role(body):
        for role, blocks in enumerate(ROLE_BLOCKS):
            @pl.when(chip == role)
            def _():
                body(blocks)

    def scores(blk, h):
        kk = kbuf[h, pl.ds(pl.multiple_of(chip_of[blk] * pair, pair), pair), :]
        return lax.dot_general(qt[h], kk, (((1,), (1,)), ((), ())), preferred_element_type=F32)

    def score_own(h):
        s = scores(OWN, h)
        q_pos = lax.broadcasted_iota(jnp.int32, (rows, pair), 0) % tokens + core * tokens
        k_pos = lax.broadcasted_iota(jnp.int32, (rows, pair), 1)
        s = jnp.where(k_pos <= q_pos, s, -jnp.inf)
        s_buf[OWN, h] = s
        mp[h] = jnp.maximum(s[:, :tokens], s[:, tokens:])

    def score_other(blk, h):
        s = scores(blk, h)
        s_buf[blk, h] = s
        mp[h] = jnp.maximum(mp[h], jnp.maximum(s[:, :tokens], s[:, tokens:]))

    needed = {X: ix == 1, Y: iy == 1, Z: iy == 1}

    def scores_of(blk, unit):
        h0, n, _ = K_UNITS[unit]

        @pl.when(needed[blk])
        def _():
            for h in range(h0, h0 + n):
                score_other(blk, h)

    loads[0].wait()
    split_heads(k_raw, num_kv, put_k)
    pl.semaphore_wait(barrier, 3)
    own_link(0, 0)
    own_link(1, 1)
    own_link(1, 0)
    own_link(0, 1)
    for u in range(NK):
        send(u, ME, dev_p, PT)
    loads[1].wait()
    split_heads(v_raw, num_kv, put_v)
    loads[2].wait()
    split_heads(q_raw, num_heads, put_q)
    for u in range(NK):
        arrive(u, PT)
    for h in range(num_kv):
        score_own(h)

    arrive(0, X)
    relay(0, X)
    arrive(1, Y)
    relay(1, Y)
    share(0, X)
    share(1, Y)
    for a, b in ((0, 1), (1, 0), (2, 3), (3, 2)):
        own_link(NK + a, 0)
        own_link(NK + b, 1)
    for u in range(NV):
        send(NK + u, ME, dev_p, PT)
    arrive(0, PX)
    scores_of(X, 0)
    arrive(1, PY)
    scores_of(Y, 1)
    arrive(1, X)
    share(1, X)
    arrive(0, Y)
    share(0, Y)
    arrive(1, PX)
    scores_of(X, 1)
    arrive(0, PY)
    scores_of(Y, 0)
    arrive(0, Z)
    share(0, Z)
    arrive(1, Z)
    share(1, Z)
    arrive(0, PZ)
    scores_of(Z, 0)
    arrive(1, PZ)
    scores_of(Z, 1)

    log2_scale = dim ** -0.5 * math.log2(math.e)
    step_rows = 64

    def row_max(h):
        mp[h] = jnp.broadcast_to(jnp.max(mp[h], axis=-1, keepdims=True) * log2_scale, (rows, tokens))

    def probs(h, blocks):
        for r0 in range(0, rows, step_rows):
            r = pl.ds(r0, step_rows)
            m = mp[h, r, :]
            total = None
            for blk in blocks:
                for c0 in (0, tokens):
                    p = jnp.exp2(s_buf[blk, h, r, pl.ds(c0, tokens)] * log2_scale - m)
                    p_buf[blk, h, r, pl.ds(c0, tokens)] = p.astype(BF16)
                    total = p if total is None else total + p
            lsum[h, r, :] = total

    def row_sum(h):
        lsum[h] = jnp.broadcast_to(1.0 / jnp.sum(lsum[h], axis=-1, keepdims=True), (rows, dim))

    def weighted(h, blocks):
        total = None
        for blk in blocks:
            vv = vbuf[h, pl.ds(pl.multiple_of(chip_of[blk] * pair, pair), pair), :]
            part = lax.dot_general(p_buf[blk, h], vv, (((1,), (0,)), ((), ())), preferred_element_type=F32)
            total = part if total is None else total + part
        return total

    def near(h, blocks):
        acc[h] = weighted(h, [blk for blk in blocks if blk != Z])

    def last(h, blocks):
        out = acc[h] if Z not in blocks else acc[h] + weighted(h, [Z])
        out = out * lsum[h]
        for n in range(group):
            f_buf[pl.ds(h * group + n, tokens, stride=num_heads), :] = out[n * tokens : (n + 1) * tokens, :]

    def values_from_links(u):
        arrive(NK + u, X)
        arrive(NK + u, Y)
        h0, n, path = V_UNITS[u]
        for h in range(h0, h0 + n):
            relay(NK + NV + h, (X, Y)[path])
        share(NK + u, X)
        share(NK + u, Y)

    def values_from_partner(u):
        for src in (PT, PX, PY):
            arrive(NK + u, src)

    def stage(h):
        def body(blocks):
            if h == 0:
                row_max(0)
            if h + 1 < num_kv:
                row_max(h + 1)
            if h < num_kv:
                probs(h, blocks)
            if h > 0:
                row_sum(h - 1)

        by_role(body)

    def near_stage(u):
        h0, n, _ = V_UNITS[u]

        def body(blocks):
            for h in range(h0, h0 + n):
                near(h, blocks)

        by_role(body)

    for u in range(NV):
        stage(2 * u)
        values_from_links(u)
        stage(2 * u + 1)
        if u > 0:
            values_from_partner(u - 1)
            near_stage(u - 1)
    stage(num_kv)
    values_from_partner(NV - 1)
    near_stage(NV - 1)
    order = (0, 2, 1, 3, 4, 6, 5, 7)
    for i, h in enumerate(order):
        arrive(NK + NV + h, Z)
        share(NK + NV + h, Z)
        if i > 0:
            g = order[i - 1]
            arrive(NK + NV + g, PZ)
            by_role(lambda blocks: last(g, blocks))
    arrive(NK + NV + order[-1], PZ)
    by_role(lambda blocks: last(order[-1], blocks))

    def narrow(i, carry):
        t = pl.multiple_of(i * 16, 16)
        o_ref[pl.ds(t, 16)] = f_buf[pl.ds(pl.multiple_of(t * num_heads, 16 * num_heads), 16 * num_heads), :].reshape(16, num_heads, dim).astype(BF16)
        return carry

    lax.fori_loop(0, tokens // 16, narrow, 0)
    for copy in sends:
        copy.wait_send()


def solution(mesh):
    seq_spec = P(("batch", "cx", "cy"), None, None)
    ranks = mesh.shape["cx"] * mesh.shape["cy"]

    def local(q, k, v):
        tokens, heads, dim = q.shape
        kv = k.shape[1]
        rows = heads // kv * tokens
        hbm = pl.BlockSpec(memory_space=pltpu.HBM)
        return pl.pallas_call(
            kernel,
            out_shape=jax.ShapeDtypeStruct(q.shape, q.dtype),
            in_specs=[hbm, hbm, hbm],
            out_specs=pl.BlockSpec(memory_space=pltpu.VMEM),
            scratch_shapes=[
                pltpu.VMEM((kv, ranks * tokens, dim), BF16),
                pltpu.VMEM((kv, ranks * tokens, dim), BF16),
                pltpu.VMEM((kv, rows, dim), BF16),
                pltpu.VMEM((4, kv, rows, 2 * tokens), F32),
                pltpu.VMEM((4, kv, rows, 2 * tokens), BF16),
                pltpu.VMEM((kv, rows, dim), F32),
                pltpu.VMEM((kv, rows, dim), F32),
                pltpu.VMEM((kv, rows, dim), F32),
                pltpu.VMEM((tokens, heads, dim), BF16),
                pltpu.VMEM((tokens, kv, dim), BF16),
                pltpu.VMEM((tokens, kv, dim), BF16),
                pltpu.VMEM((tokens * heads, dim), F32),
                pltpu.SemaphoreType.DMA((3,)),
                pltpu.SemaphoreType.DMA((72,)),
                pltpu.SemaphoreType.DMA((7 * NU,)),
            ],
            compiler_params=pltpu.CompilerParams(collective_id=0, has_side_effects=True, vmem_limit_bytes=54 * 2**20),
        )(q, k, v)

    return jax.shard_map(local, mesh=mesh, in_specs=(seq_spec, seq_spec, seq_spec), out_specs=seq_spec, check_vma=False)
```

```python
import math

import jax
import jax.numpy as jnp
from jax import lax
from jax.experimental import pallas as pl
from jax.experimental.pallas import tpu as pltpu
from jax.sharding import PartitionSpec as P

MESH = pl.DeviceIdType.MESH
F32 = jnp.float32
BF16 = jnp.bfloat16

K_UNITS = ((0, 4, 0), (4, 4, 1))
V_UNITS = ((0, 2, 0), (2, 2, 1), (4, 2, 0), (6, 2, 1))
W_UNITS = tuple((h, 1, (h // 2) % 2) for h in range(8))
NK, NV, NW = len(K_UNITS), len(V_UNITS), len(W_UNITS)
UNITS = K_UNITS + V_UNITS + W_UNITS
NU = len(UNITS)
X, Y, Z, OWN = range(4)
PT, PX, PY, PZ = 3, 4, 5, 6
ME = 7
ROLE_BLOCKS = ((OWN,), (OWN, X), (OWN, Y, Z), (OWN, X, Y, Z))


def kernel(q_hbm, k_hbm, v_hbm, o_ref, kbuf, vbuf, qt, s_buf, p_buf, mp, lsum, acc, q_raw, k_raw, v_raw, f_buf, lsem, ssem, rsem):
    tokens, num_heads, dim = q_hbm.shape
    num_kv = k_hbm.shape[1]
    group = num_heads // num_kv
    rows = group * tokens
    pair = 2 * tokens
    iy, cy = lax.axis_index("cx"), lax.axis_index("cy")
    ix, core = cy // 2, cy % 2
    chip = iy * 2 + ix
    cy_x = (cy + 2) % 4
    cy_p = cy + 1 - 2 * core
    cy_xp = (cy_p + 2) % 4
    iy_o = 1 - iy
    rank_of = {ME: iy * 4 + cy, X: iy * 4 + cy_x, Y: iy_o * 4 + cy, Z: iy_o * 4 + cy_x, PT: iy * 4 + cy_p, PX: iy * 4 + cy_xp, PY: iy_o * 4 + cy_p, PZ: iy_o * 4 + cy_xp}
    dev_x, dev_y, dev_p = (0, iy, cy_x), (0, iy_o, cy), (0, iy, cy_p)
    chip_of = {X: iy * 2 + 1 - ix, Y: iy_o * 2 + ix, Z: iy_o * 2 + 1 - ix, OWN: chip}

    loads = [pltpu.make_async_copy(k_hbm, k_raw, lsem.at[0]), pltpu.make_async_copy(v_hbm, v_raw, lsem.at[1]), pltpu.make_async_copy(q_hbm, q_raw, lsem.at[2])]
    for load in loads:
        load.start()
    barrier = pltpu.get_barrier_semaphore()
    pl.semaphore_signal(barrier, inc=1, device_id=dev_p, device_id_type=MESH)
    pl.semaphore_signal(barrier, inc=1, device_id=dev_x, device_id_type=MESH)

    @pl.when(iy == 1)
    def _():
        pl.semaphore_signal(barrier, inc=1, device_id=dev_y, device_id_type=MESH)


    def split_heads(raw, heads, put):
        step = 32

        def widen(i, carry):
            t = pl.multiple_of(i * step, step)
            f_buf[pl.ds(pl.multiple_of(t * heads, step * heads), step * heads), :] = raw[pl.ds(t, step)].astype(F32).reshape(step * heads, dim)
            return carry

        lax.fori_loop(0, tokens // step, widen, 0)
        for h in range(heads):
            put(h, f_buf[pl.ds(h, tokens, stride=heads), :].astype(BF16))

    my_rows = pl.ds(pl.multiple_of(rank_of[ME] * tokens, tokens), tokens)

    def put_k(h, val):
        kbuf[h, my_rows, :] = val

    def put_v(h, val):
        vbuf[h, my_rows, :] = val

    def put_q(h, val):
        qt[h // group, pl.ds((h % group) * tokens, tokens), :] = val

    top, low, right, left = iy == 1, iy == 0, ix == 1, ix == 0
    not_third, not_last = chip != 2, chip != 3
    sends = []

    def when(cond, body):
        body() if cond is None else pl.when(cond)(body)

    def piece(unit, src):
        h0, n, _ = UNITS[unit]
        buf = kbuf if unit < NK else vbuf
        return buf.at[pl.ds(h0, n), pl.ds(pl.multiple_of(rank_of[src] * tokens, tokens), tokens), :]

    def send(cond, moves):
        first = len(sends)
        for i, (unit, src, dev, as_src) in enumerate(moves):
            ref = piece(unit, src)
            sends.append(pltpu.make_async_remote_copy(ref, ref, ssem.at[first + i], rsem.at[as_src * NU + unit], device_id=dev, device_id_type=MESH))
        copies = sends[first:]
        when(cond, lambda: [copy.start() for copy in copies] and None)
        drains.append((cond, copies))

    drains = []

    def arrive(cond, units, srcs):
        def body():
            for unit in units:
                for src in srcs:
                    ref = piece(unit, src)
                    pltpu.make_async_remote_copy(ref, ref, ssem.at[0], rsem.at[src * NU + unit], device_id=dev_p, device_id_type=MESH).wait_recv()

        when(cond, body)

    def path(unit):
        return UNITS[unit][2]

    def own_x(unit):
        send(left if path(unit) else not_last, [(unit, ME, dev_x, X)])

    def own_y(unit):
        send(low, [(unit, ME, dev_y, Y)])

    def own_partner(units):
        send(None, [(unit, ME, dev_p, PT) for unit in units])

    def arrive_x(unit):
        arrive(right if path(unit) else not_third, [unit], [X])

    def share(units, src):
        send(right if src == X else top, [(unit, src, dev_p, {X: PX, Y: PY, Z: PZ}[src]) for unit in units])

    def relay(units, src):
        send({X: low, Y: top}[src], [(unit, src, {X: dev_y, Y: dev_x}[src], Z) for unit in units])

    def by_role(body):
        for role, blocks in enumerate(ROLE_BLOCKS):
            @pl.when(chip == role)
            def _():
                body(blocks)

    def scores(blk, h):
        kk = kbuf[h, pl.ds(pl.multiple_of(chip_of[blk] * pair, pair), pair), :]
        return lax.dot_general(qt[h], kk, (((1,), (1,)), ((), ())), preferred_element_type=F32)

    def score_own(h):
        s = scores(OWN, h)
        q_pos = lax.broadcasted_iota(jnp.int32, (rows, pair), 0) % tokens + core * tokens
        k_pos = lax.broadcasted_iota(jnp.int32, (rows, pair), 1)
        s = jnp.where(k_pos <= q_pos, s, -jnp.inf)
        s_buf[OWN, h] = s
        mp[h] = jnp.maximum(s[:, :tokens], s[:, tokens:])

    def score_other(blk, h):
        s = scores(blk, h)
        s_buf[blk, h] = s
        mp[h] = jnp.maximum(mp[h], jnp.maximum(s[:, :tokens], s[:, tokens:]))

    needed = {X: ix == 1, Y: iy == 1, Z: iy == 1}

    def scores_of(blk, unit):
        h0, n, _ = K_UNITS[unit]

        @pl.when(needed[blk])
        def _():
            for h in range(h0, h0 + n):
                score_other(blk, h)

    loads[0].wait()
    split_heads(k_raw, num_kv, put_k)
    pl.when(low)(lambda: pl.semaphore_wait(barrier, 3))
    pl.when(top)(lambda: pl.semaphore_wait(barrier, 2))
    own_x(0)
    own_y(1)
    own_x(1)
    own_y(0)
    own_partner(range(NK))
    loads[1].wait()
    split_heads(v_raw, num_kv, put_v)
    loads[2].wait()
    split_heads(q_raw, num_heads, put_q)
    arrive(None, range(NK), [PT])
    for h in range(num_kv):
        score_own(h)

    arrive_x(0)
    relay([0], X)
    arrive(top, [1], [Y])
    relay([1], Y)
    share([0], X)
    share([1], Y)
    for a, b in ((0, 1), (1, 0), (2, 3), (3, 2)):
        own_x(NK + a)
        own_y(NK + b)
    own_partner(range(NK, NK + NV))
    arrive(right, [0], [PX])
    scores_of(X, 0)
    arrive(top, [1], [PY])
    scores_of(Y, 1)
    arrive_x(1)
    share([1], X)
    arrive(top, [0], [Y])
    share([0], Y)
    arrive(right, [1], [PX])
    scores_of(X, 1)
    arrive(top, [0], [PY])
    scores_of(Y, 0)
    for u in range(NK):
        arrive(top, [u], [Z])
        share([u], Z)
    for u in range(NK):
        arrive(top, [u], [PZ])
        scores_of(Z, u)

    log2_scale = dim ** -0.5 * math.log2(math.e)
    step_rows = 64

    def row_max(h):
        mp[h] = jnp.broadcast_to(jnp.max(mp[h], axis=-1, keepdims=True) * log2_scale, (rows, tokens))

    def probs(h, blocks):
        for r0 in range(0, rows, step_rows):
            r = pl.ds(r0, step_rows)
            m = mp[h, r, :]
            total = None
            for blk in blocks:
                for c0 in (0, tokens):
                    p = jnp.exp2(s_buf[blk, h, r, pl.ds(c0, tokens)] * log2_scale - m)
                    p_buf[blk, h, r, pl.ds(c0, tokens)] = p.astype(BF16)
                    total = p if total is None else total + p
            lsum[h, r, :] = total

    def row_sum(h):
        lsum[h] = jnp.broadcast_to(1.0 / jnp.sum(lsum[h], axis=-1, keepdims=True), (rows, dim))

    def weighted(h, blocks):
        total = None
        for blk in blocks:
            vv = vbuf[h, pl.ds(pl.multiple_of(chip_of[blk] * pair, pair), pair), :]
            part = lax.dot_general(p_buf[blk, h], vv, (((1,), (0,)), ((), ())), preferred_element_type=F32)
            total = part if total is None else total + part
        return total

    def near(h, blocks):
        acc[h] = weighted(h, [blk for blk in blocks if blk != Z])

    def last(h, blocks):
        out = acc[h] if Z not in blocks else acc[h] + weighted(h, [Z])
        out = out * lsum[h]
        for n in range(group):
            f_buf[pl.ds(h * group + n, tokens, stride=num_heads), :] = out[n * tokens : (n + 1) * tokens, :]

    def values_from_links(u):
        h0, n, way = V_UNITS[u]
        second = [NK + NV + h for h in range(h0, h0 + n)]
        arrive_x(NK + u)
        if way == 0:
            relay(second, X)
        share([NK + u], X)
        arrive(top, [NK + u], [Y])
        if way == 1:
            relay(second, Y)
        share([NK + u], Y)

    def values_from_partner(u):
        arrive(None, [NK + u], [PT])
        arrive(right, [NK + u], [PX])
        arrive(top, [NK + u], [PY])

    def stage(h):
        def body(blocks):
            if h == 0:
                row_max(0)
            if h + 1 < num_kv:
                row_max(h + 1)
            if h < num_kv:
                probs(h, blocks)
            if h > 0:
                row_sum(h - 1)

        by_role(body)

    def near_stage(u):
        h0, n, _ = V_UNITS[u]

        def body(blocks):
            for h in range(h0, h0 + n):
                near(h, blocks)

        by_role(body)

    for u in range(NV):
        stage(2 * u)
        values_from_links(u)
        stage(2 * u + 1)
        if u > 0:
            values_from_partner(u - 1)
            near_stage(u - 1)
    stage(num_kv)
    values_from_partner(NV - 1)
    near_stage(NV - 1)
    order = (0, 2, 1, 3, 4, 6, 5, 7)
    for i, h in enumerate(order):
        arrive(top, [NK + NV + h], [Z])
        share([NK + NV + h], Z)
        if i > 0:
            g = order[i - 1]
            arrive(top, [NK + NV + g], [PZ])
            by_role(lambda blocks: last(g, blocks))
    arrive(top, [NK + NV + order[-1]], [PZ])
    by_role(lambda blocks: last(order[-1], blocks))

    def narrow(i, carry):
        t = pl.multiple_of(i * 16, 16)
        o_ref[pl.ds(t, 16)] = f_buf[pl.ds(pl.multiple_of(t * num_heads, 16 * num_heads), 16 * num_heads), :].reshape(16, num_heads, dim).astype(BF16)
        return carry

    lax.fori_loop(0, tokens // 16, narrow, 0)
    for cond, copies in drains:
        when(cond, lambda: [copy.wait_send() for copy in copies] and None)


def solution(mesh):
    seq_spec = P(("batch", "cx", "cy"), None, None)
    ranks = mesh.shape["cx"] * mesh.shape["cy"]

    def local(q, k, v):
        tokens, heads, dim = q.shape
        kv = k.shape[1]
        rows = heads // kv * tokens
        hbm = pl.BlockSpec(memory_space=pltpu.HBM)
        return pl.pallas_call(
            kernel,
            out_shape=pltpu.VMEM(q.shape, q.dtype),
            in_specs=[hbm, hbm, hbm],
            out_specs=pl.BlockSpec(memory_space=pltpu.VMEM),
            scratch_shapes=[
                pltpu.VMEM((kv, ranks * tokens, dim), BF16),
                pltpu.VMEM((kv, ranks * tokens, dim), BF16),
                pltpu.VMEM((kv, rows, dim), BF16),
                pltpu.VMEM((4, kv, rows, 2 * tokens), F32),
                pltpu.VMEM((4, kv, rows, 2 * tokens), BF16),
                pltpu.VMEM((kv, rows, dim), F32),
                pltpu.VMEM((kv, rows, dim), F32),
                pltpu.VMEM((kv, rows, dim), F32),
                pltpu.VMEM((tokens, heads, dim), BF16),
                pltpu.VMEM((tokens, kv, dim), BF16),
                pltpu.VMEM((tokens, kv, dim), BF16),
                pltpu.VMEM((tokens * heads, dim), F32),
                pltpu.SemaphoreType.DMA((3,)),
                pltpu.SemaphoreType.DMA((72,)),
                pltpu.SemaphoreType.DMA((7 * NU,)),
            ],
            compiler_params=pltpu.CompilerParams(collective_id=0, has_side_effects=True, vmem_limit_bytes=54 * 2**20),
        )(*[pltpu.with_memory_space_constraint(a, pltpu.HBM) for a in (q, k, v)])

    return jax.shard_map(local, mesh=mesh, in_specs=(seq_spec, seq_spec, seq_spec), out_specs=seq_spec, check_vma=False)
```

```python
import math

import jax
import jax.numpy as jnp
from jax import lax
from jax.experimental import pallas as pl
from jax.experimental.pallas import tpu as pltpu
from jax.sharding import PartitionSpec as P

MESH = pl.DeviceIdType.MESH
F32 = jnp.float32
BF16 = jnp.bfloat16

K_UNITS = ((0, 4, 0), (4, 4, 1))
V_UNITS = ((0, 2, 0), (2, 2, 1), (4, 2, 0), (6, 2, 1))
W_UNITS = tuple((h, 1, (h // 2) % 2) for h in range(8))
NK, NV, NW = len(K_UNITS), len(V_UNITS), len(W_UNITS)
UNITS = K_UNITS + V_UNITS + W_UNITS
NU = len(UNITS)
X, Y, Z, OWN = range(4)
PT, PX, PY, PZ = 3, 4, 5, 6
ME = 7
ROLE_BLOCKS = ((OWN,), (OWN, X), (OWN, Y, Z), (OWN, X, Y, Z))


def kernel(q_hbm, k_hbm, v_hbm, o_ref, kbuf, vbuf, qt, s_buf, p_buf, mp, mz, lsum, acc, q_raw, k_raw, v_raw, f_buf, lsem, ssem, rsem):
    tokens, num_heads, dim = q_hbm.shape
    num_kv = k_hbm.shape[1]
    group = num_heads // num_kv
    rows = group * tokens
    pair = 2 * tokens
    iy, cy = lax.axis_index("cx"), lax.axis_index("cy")
    ix, core = cy // 2, cy % 2
    chip = iy * 2 + ix
    cy_x = (cy + 2) % 4
    cy_p = cy + 1 - 2 * core
    cy_xp = (cy_p + 2) % 4
    iy_o = 1 - iy
    rank_of = {ME: iy * 4 + cy, X: iy * 4 + cy_x, Y: iy_o * 4 + cy, Z: iy_o * 4 + cy_x, PT: iy * 4 + cy_p, PX: iy * 4 + cy_xp, PY: iy_o * 4 + cy_p, PZ: iy_o * 4 + cy_xp}
    dev_x, dev_y, dev_p = (0, iy, cy_x), (0, iy_o, cy), (0, iy, cy_p)
    chip_of = {X: iy * 2 + 1 - ix, Y: iy_o * 2 + ix, Z: iy_o * 2 + 1 - ix, OWN: chip}

    loads = [pltpu.make_async_copy(k_hbm, k_raw, lsem.at[0]), pltpu.make_async_copy(v_hbm, v_raw, lsem.at[1]), pltpu.make_async_copy(q_hbm, q_raw, lsem.at[2])]
    for load in loads:
        load.start()
    barrier = pltpu.get_barrier_semaphore()
    pl.semaphore_signal(barrier, inc=1, device_id=dev_p, device_id_type=MESH)
    pl.semaphore_signal(barrier, inc=1, device_id=dev_x, device_id_type=MESH)

    @pl.when(iy == 1)
    def _():
        pl.semaphore_signal(barrier, inc=1, device_id=dev_y, device_id_type=MESH)


    def split_heads(raw, heads, put):
        step = 32

        def widen(i, carry):
            t = pl.multiple_of(i * step, step)
            f_buf[pl.ds(pl.multiple_of(t * heads, step * heads), step * heads), :] = raw[pl.ds(t, step)].astype(F32).reshape(step * heads, dim)
            return carry

        lax.fori_loop(0, tokens // step, widen, 0)
        for h in range(heads):
            put(h, f_buf[pl.ds(h, tokens, stride=heads), :].astype(BF16))

    my_rows = pl.ds(pl.multiple_of(rank_of[ME] * tokens, tokens), tokens)

    def put_k(h, val):
        kbuf[h, my_rows, :] = val

    def put_v(h, val):
        vbuf[h, my_rows, :] = val

    def put_q(h, val):
        qt[h // group, pl.ds((h % group) * tokens, tokens), :] = val

    top, low, right, left = iy == 1, iy == 0, ix == 1, ix == 0
    not_third, not_last = chip != 2, chip != 3
    sends = []

    def when(cond, body):
        body() if cond is None else pl.when(cond)(body)

    def piece(unit, src):
        h0, n, _ = UNITS[unit]
        buf = kbuf if unit < NK else vbuf
        return buf.at[pl.ds(h0, n), pl.ds(pl.multiple_of(rank_of[src] * tokens, tokens), tokens), :]

    def send(cond, moves):
        first = len(sends)
        for i, (unit, src, dev, as_src) in enumerate(moves):
            ref = piece(unit, src)
            sends.append(pltpu.make_async_remote_copy(ref, ref, ssem.at[first + i], rsem.at[as_src * NU + unit], device_id=dev, device_id_type=MESH))
        copies = sends[first:]
        when(cond, lambda: [copy.start() for copy in copies] and None)
        drains.append((cond, copies))

    drains = []

    def arrive(cond, units, srcs):
        def body():
            for unit in units:
                for src in srcs:
                    ref = piece(unit, src)
                    pltpu.make_async_remote_copy(ref, ref, ssem.at[0], rsem.at[src * NU + unit], device_id=dev_p, device_id_type=MESH).wait_recv()

        when(cond, body)

    def path(unit):
        return UNITS[unit][2]

    def own_x(unit):
        send(left if path(unit) else not_last, [(unit, ME, dev_x, X)])

    def own_y(unit):
        send(low, [(unit, ME, dev_y, Y)])

    def own_values(first):
        if first:
            for u in (0, 2, 1, 3):
                send(chip == 0, [(NK + u, ME, dev_x, X)])
            for u in (1, 3):
                send(chip == 0, [(NK + u, ME, dev_y, Y)])
            return
        for a, b in ((1, 1), (3, 3), (0, 0), (2, 2)):
            send(chip == 2 if path(NK + a) else (chip + 1) // 2 == 1, [(NK + a, ME, dev_x, X)])
            send(chip == 1 if path(NK + b) else low, [(NK + b, ME, dev_y, Y)])

    def own_partner(units):
        send(None, [(unit, ME, dev_p, PT) for unit in units])

    def arrive_x(unit):
        arrive(right if path(unit) else not_third, [unit], [X])

    def share(units, src):
        send(right if src == X else top, [(unit, src, dev_p, {X: PX, Y: PY, Z: PZ}[src]) for unit in units])

    def relay(units, src):
        send({X: low, Y: top}[src], [(unit, src, {X: dev_y, Y: dev_x}[src], Z) for unit in units])

    def by_role(body):
        for role, blocks in enumerate(ROLE_BLOCKS):
            @pl.when(chip == role)
            def _():
                body(blocks)

    def scores(blk, h):
        kk = kbuf[h, pl.ds(pl.multiple_of(chip_of[blk] * pair, pair), pair), :]
        return lax.dot_general(qt[h], kk, (((1,), (1,)), ((), ())), preferred_element_type=F32)

    def score_own(h):
        s = scores(OWN, h)
        q_pos = lax.broadcasted_iota(jnp.int32, (rows, pair), 0) % tokens + core * tokens
        k_pos = lax.broadcasted_iota(jnp.int32, (rows, pair), 1)
        s = jnp.where(k_pos <= q_pos, s, -jnp.inf)
        s_buf[OWN, h] = s
        mp[h] = jnp.maximum(s[:, :tokens], s[:, tokens:])

    def score_other(blk, h):
        s = scores(blk, h)
        s_buf[blk, h] = s
        mp[h] = jnp.maximum(mp[h], jnp.maximum(s[:, :tokens], s[:, tokens:]))

    needed = {X: ix == 1, Y: iy == 1}

    def scores_of(blk, unit):
        h0, n, _ = K_UNITS[unit]

        @pl.when(needed[blk])
        def _():
            for h in range(h0, h0 + n):
                score_other(blk, h)

    loads[0].wait()
    split_heads(k_raw, num_kv, put_k)
    pl.when(low)(lambda: pl.semaphore_wait(barrier, 3))
    pl.when(top)(lambda: pl.semaphore_wait(barrier, 2))
    own_x(0)
    own_y(1)
    own_x(1)
    own_y(0)
    own_partner(range(NK))
    loads[1].wait()
    split_heads(v_raw, num_kv, put_v)
    own_values(True)
    loads[2].wait()
    split_heads(q_raw, num_heads, put_q)
    arrive(None, range(NK), [PT])
    for h in range(num_kv):
        score_own(h)

    arrive_x(0)
    relay([0], X)
    arrive(top, [1], [Y])
    relay([1], Y)
    share([0], X)
    share([1], Y)
    own_values(False)
    own_partner(range(NK, NK + NV))
    arrive(right, [0], [PX])
    scores_of(X, 0)
    arrive(top, [1], [PY])
    scores_of(Y, 1)
    arrive_x(1)
    share([1], X)
    arrive(top, [0], [Y])
    share([0], Y)
    arrive(right, [1], [PX])
    scores_of(X, 1)
    arrive(top, [0], [PY])
    scores_of(Y, 0)
    log2_scale = dim ** -0.5 * math.log2(math.e)
    step_rows = 64

    def row_max(h):
        mp[h] = jnp.broadcast_to(jnp.max(mp[h], axis=-1, keepdims=True) * log2_scale, (rows, tokens))

    def probs(h, blocks):
        for r0 in range(0, rows, step_rows):
            r = pl.ds(r0, step_rows)
            m = mp[h, r, :]
            total = None
            for blk in blocks:
                for c0 in (0, tokens):
                    p = jnp.exp2(s_buf[blk, h, r, pl.ds(c0, tokens)] * log2_scale - m)
                    p_buf[blk, h, r, pl.ds(c0, tokens)] = p.astype(BF16)
                    total = p if total is None else total + p
            lsum[h, r, :] = total

    def row_sum(h):
        lsum[h] = jnp.broadcast_to(1.0 / jnp.sum(lsum[h], axis=-1, keepdims=True), (rows, dim))

    def far_scores(h):
        s = scores(Z, h)
        s_buf[Z, h] = s
        mz[h] = jnp.maximum(s[:, :tokens], s[:, tokens:])

    def far_probs(h):
        for r0 in range(0, rows, step_rows):
            r = pl.ds(r0, step_rows)
            old = mp[h, r, :]
            m = jnp.maximum(old, jnp.broadcast_to(jnp.max(mz[h, r, :], axis=-1, keepdims=True) * log2_scale, (step_rows, tokens)))
            factor = jnp.exp2(old - m)
            mp[h, r, :] = factor
            total = lsum[h, r, :] * factor
            for c0 in (0, tokens):
                p = jnp.exp2(s_buf[Z, h, r, pl.ds(c0, tokens)] * log2_scale - m)
                p_buf[Z, h, r, pl.ds(c0, tokens)] = p.astype(BF16)
                total = total + p
            lsum[h, r, :] = total

    def weighted(h, blocks):
        total = None
        for blk in blocks:
            vv = vbuf[h, pl.ds(pl.multiple_of(chip_of[blk] * pair, pair), pair), :]
            part = lax.dot_general(p_buf[blk, h], vv, (((1,), (0,)), ((), ())), preferred_element_type=F32)
            total = part if total is None else total + part
        return total

    def near(h, blocks):
        acc[h] = weighted(h, [blk for blk in blocks if blk != Z])

    def last(h, blocks):
        out = acc[h] if Z not in blocks else acc[h] * mp[h] + weighted(h, [Z])
        out = out * lsum[h]
        for n in range(group):
            f_buf[pl.ds(h * group + n, tokens, stride=num_heads), :] = out[n * tokens : (n + 1) * tokens, :]

    def values_from_links(u):
        h0, n, way = V_UNITS[u]
        second = [NK + NV + h for h in range(h0, h0 + n)]
        arrive(top, [NK + u], [Y])
        if way == 1:
            relay(second, Y)
        share([NK + u], Y)
        arrive_x(NK + u)
        if way == 0:
            relay(second, X)
        share([NK + u], X)

    def values_from_partner(u):
        arrive(None, [NK + u], [PT])
        arrive(right, [NK + u], [PX])
        arrive(top, [NK + u], [PY])

    def stage(heads):
        def body(blocks):
            for h in heads:
                if h == 0:
                    row_max(0)
                if h + 1 < num_kv:
                    row_max(h + 1)
                probs(h, [blk for blk in blocks if blk != Z])

        by_role(body)

    def far_stage(heads):
        def body(blocks):
            for h in heads:
                if Z in blocks:
                    if h == 0:
                        far_scores(0)
                    if h + 1 < num_kv:
                        far_scores(h + 1)
                    if h < num_kv:
                        far_probs(h)
                if h > 0:
                    row_sum(h - 1)

        by_role(body)

    def second_hop(heads):
        for h in heads:
            arrive(top, [NK + NV + h], [Z])
            share([NK + NV + h], Z)

    def last_stage(heads):
        arrive(top, [NK + NV + h for h in heads], [PZ])

        def body(blocks):
            for h in heads:
                last(h, blocks)

        by_role(body)

    def near_stage(u):
        h0, n, _ = V_UNITS[u]

        def body(blocks):
            for h in range(h0, h0 + n):
                near(h, blocks)

        by_role(body)

    stage((0, 1))
    for u in range(NK):
        arrive(top, [u], [Z])
        share([u], Z)
    stage((2, 3))
    stage((4, 5))
    stage((6, 7))
    arrive(top, range(NK), [PZ])
    turn = (1, 3, 0, 2)
    for i, u in enumerate(turn):
        values_from_links(u)
        far_stage((2 * i, 2 * i + 1) if i < NV - 1 else (2 * i, 2 * i + 1, num_kv))
        if i > 0:
            values_from_partner(turn[i - 1])
            near_stage(turn[i - 1])
    second_hop((0, 2))
    second_hop((1, 3))
    values_from_partner(turn[-1])
    near_stage(turn[-1])
    second_hop((4, 6))
    last_stage((0, 2))
    second_hop((5, 7))
    last_stage((1, 3))
    last_stage((4, 6))
    last_stage((5, 7))

    def narrow(i, carry):
        t = pl.multiple_of(i * 16, 16)
        o_ref[pl.ds(t, 16)] = f_buf[pl.ds(pl.multiple_of(t * num_heads, 16 * num_heads), 16 * num_heads), :].reshape(16, num_heads, dim).astype(BF16)
        return carry

    lax.fori_loop(0, tokens // 16, narrow, 0)
    for cond, copies in drains:
        when(cond, lambda: [copy.wait_send() for copy in copies] and None)


def solution(mesh):
    seq_spec = P(("batch", "cx", "cy"), None, None)
    ranks = mesh.shape["cx"] * mesh.shape["cy"]

    def local(q, k, v):
        tokens, heads, dim = q.shape
        kv = k.shape[1]
        rows = heads // kv * tokens
        hbm = pl.BlockSpec(memory_space=pltpu.HBM)
        return pl.pallas_call(
            kernel,
            out_shape=pltpu.VMEM(q.shape, q.dtype),
            in_specs=[hbm, hbm, hbm],
            out_specs=pl.BlockSpec(memory_space=pltpu.VMEM),
            scratch_shapes=[
                pltpu.VMEM((kv, ranks * tokens, dim), BF16),
                pltpu.VMEM((kv, ranks * tokens, dim), BF16),
                pltpu.VMEM((kv, rows, dim), BF16),
                pltpu.VMEM((4, kv, rows, 2 * tokens), F32),
                pltpu.VMEM((4, kv, rows, 2 * tokens), BF16),
                pltpu.VMEM((kv, rows, dim), F32),
                pltpu.VMEM((kv, rows, dim), F32),
                pltpu.VMEM((kv, rows, dim), F32),
                pltpu.VMEM((kv, rows, dim), F32),
                pltpu.VMEM((tokens, heads, dim), BF16),
                pltpu.VMEM((tokens, kv, dim), BF16),
                pltpu.VMEM((tokens, kv, dim), BF16),
                pltpu.VMEM((tokens * heads, dim), F32),
                pltpu.SemaphoreType.DMA((3,)),
                pltpu.SemaphoreType.DMA((80,)),
                pltpu.SemaphoreType.DMA((7 * NU,)),
            ],
            compiler_params=pltpu.CompilerParams(collective_id=0, has_side_effects=True, vmem_limit_bytes=57 * 2**20),
        )(*[pltpu.with_memory_space_constraint(a, pltpu.HBM) for a in (q, k, v)])

    return jax.shard_map(local, mesh=mesh, in_specs=(seq_spec, seq_spec, seq_spec), out_specs=seq_spec, check_vma=False)
```

```python
import math

import jax
import jax.numpy as jnp
from jax import lax
from jax.experimental import pallas as pl
from jax.experimental.pallas import tpu as pltpu
from jax.sharding import PartitionSpec as P

MESH = pl.DeviceIdType.MESH
F32 = jnp.float32
BF16 = jnp.bfloat16

K_UNITS = ((0, 4, 0), (4, 4, 1))
V_UNITS = ((0, 2, 0), (2, 2, 1), (4, 2, 0), (6, 2, 1))
W_UNITS = tuple((h, 1, (h // 2) % 2) for h in range(8))
NK, NV, NW = len(K_UNITS), len(V_UNITS), len(W_UNITS)
UNITS = K_UNITS + V_UNITS + W_UNITS
NU = len(UNITS)
X, Y, Z, OWN = range(4)
PT, PX, PY, PZ = 3, 4, 5, 6
ME = 7
ROLE_BLOCKS = ((OWN,), (OWN, X), (OWN, Y, Z), (OWN, X, Y, Z))


def kernel(q_hbm, k_hbm, v_hbm, o_ref, kbuf, vbuf, qt, s_buf, p_buf, mp, mz, lsum, acc, q_raw, k_raw, v_raw, f_buf, lsem, ssem, rsem):
    tokens, num_heads, dim = q_hbm.shape
    num_kv = k_hbm.shape[1]
    group = num_heads // num_kv
    rows = group * tokens
    pair = 2 * tokens
    iy, cy = lax.axis_index("cx"), lax.axis_index("cy")
    ix, core = cy // 2, cy % 2
    chip = iy * 2 + ix
    cy_x = (cy + 2) % 4
    cy_p = cy + 1 - 2 * core
    cy_xp = (cy_p + 2) % 4
    iy_o = 1 - iy
    rank_of = {ME: iy * 4 + cy, X: iy * 4 + cy_x, Y: iy_o * 4 + cy, Z: iy_o * 4 + cy_x, PT: iy * 4 + cy_p, PX: iy * 4 + cy_xp, PY: iy_o * 4 + cy_p, PZ: iy_o * 4 + cy_xp}
    dev_x, dev_y, dev_p = (0, iy, cy_x), (0, iy_o, cy), (0, iy, cy_p)
    chip_of = {X: iy * 2 + 1 - ix, Y: iy_o * 2 + ix, Z: iy_o * 2 + 1 - ix, OWN: chip}

    loads = [pltpu.make_async_copy(k_hbm, k_raw, lsem.at[0]), pltpu.make_async_copy(v_hbm, v_raw, lsem.at[1]), pltpu.make_async_copy(q_hbm, q_raw, lsem.at[2])]
    for load in loads:
        load.start()
    barrier = pltpu.get_barrier_semaphore()
    pl.semaphore_signal(barrier, inc=1, device_id=dev_p, device_id_type=MESH)
    pl.semaphore_signal(barrier, inc=1, device_id=dev_x, device_id_type=MESH)

    @pl.when(iy == 1)
    def _():
        pl.semaphore_signal(barrier, inc=1, device_id=dev_y, device_id_type=MESH)


    def split_heads(raw, heads, put):
        step = 32

        def widen(i, carry):
            t = pl.multiple_of(i * step, step)
            f_buf[pl.ds(pl.multiple_of(t * heads, step * heads), step * heads), :] = raw[pl.ds(t, step)].astype(F32).reshape(step * heads, dim)
            return carry

        lax.fori_loop(0, tokens // step, widen, 0)
        for h in range(heads):
            put(h, f_buf[pl.ds(h, tokens, stride=heads), :].astype(BF16))

    my_rows = pl.ds(pl.multiple_of(rank_of[ME] * tokens, tokens), tokens)

    def put_k(h, val):
        kbuf[h, my_rows, :] = val

    def put_v(h, val):
        vbuf[h, my_rows, :] = val

    def put_q(h, val):
        qt[h // group, pl.ds((h % group) * tokens, tokens), :] = val

    top, low, right, left = iy == 1, iy == 0, ix == 1, ix == 0
    not_third, not_last = chip != 2, chip != 3
    sends = []

    def when(cond, body):
        body() if cond is None else pl.when(cond)(body)

    def piece(unit, src):
        h0, n, _ = UNITS[unit]
        buf = kbuf if unit < NK else vbuf
        return buf.at[pl.ds(h0, n), pl.ds(pl.multiple_of(rank_of[src] * tokens, tokens), tokens), :]

    def send(cond, moves):
        first = len(sends)
        for i, (unit, src, dev, as_src) in enumerate(moves):
            ref = piece(unit, src)
            sends.append(pltpu.make_async_remote_copy(ref, ref, ssem.at[first + i], rsem.at[as_src * NU + unit], device_id=dev, device_id_type=MESH))
        copies = sends[first:]
        when(cond, lambda: [copy.start() for copy in copies] and None)
        drains.append((cond, copies))

    drains = []

    def arrive(cond, units, srcs):
        def body():
            for unit in units:
                for src in srcs:
                    ref = piece(unit, src)
                    pltpu.make_async_remote_copy(ref, ref, ssem.at[0], rsem.at[src * NU + unit], device_id=dev_p, device_id_type=MESH).wait_recv()

        when(cond, body)

    def path(unit):
        return UNITS[unit][2]

    def own_x(unit):
        send(left if path(unit) else not_last, [(unit, ME, dev_x, X)])

    def own_y(unit):
        send(low, [(unit, ME, dev_y, Y)])

    def own_values(first):
        if first:
            for u in (0, 2, 1, 3):
                send(chip == 0, [(NK + u, ME, dev_x, X)])
            send(chip == 0, [(NK + 1, ME, dev_y, Y)])
            return
        for a, b in ((1, 1), (3, 3), (0, 0), (2, 2)):
            send(chip == 2 if path(NK + a) else (chip + 1) // 2 == 1, [(NK + a, ME, dev_x, X)])
            send(chip == 1 if b == 1 else low, [(NK + b, ME, dev_y, Y)])

    def own_partner(units):
        send(None, [(unit, ME, dev_p, PT) for unit in units])

    def arrive_x(unit):
        arrive(right if path(unit) else not_third, [unit], [X])

    def share(units, src):
        send(right if src == X else top, [(unit, src, dev_p, {X: PX, Y: PY, Z: PZ}[src]) for unit in units])

    def relay(units, src):
        send({X: low, Y: top}[src], [(unit, src, {X: dev_y, Y: dev_x}[src], Z) for unit in units])

    def by_role(body):
        for role, blocks in enumerate(ROLE_BLOCKS):
            @pl.when(chip == role)
            def _():
                body(blocks)

    def scores(blk, h):
        kk = kbuf[h, pl.ds(pl.multiple_of(chip_of[blk] * pair, pair), pair), :]
        return lax.dot_general(qt[h], kk, (((1,), (1,)), ((), ())), preferred_element_type=F32)

    def score_own(h):
        s = scores(OWN, h)
        q_pos = lax.broadcasted_iota(jnp.int32, (rows, pair), 0) % tokens + core * tokens
        k_pos = lax.broadcasted_iota(jnp.int32, (rows, pair), 1)
        s = jnp.where(k_pos <= q_pos, s, -jnp.inf)
        s_buf[OWN, h] = s
        mp[h] = jnp.maximum(s[:, :tokens], s[:, tokens:])

    def score_other(blk, h):
        s = scores(blk, h)
        s_buf[blk, h] = s
        mp[h] = jnp.maximum(mp[h], jnp.maximum(s[:, :tokens], s[:, tokens:]))

    needed = {X: ix == 1, Y: iy == 1}

    def scores_of(blk, unit):
        h0, n, _ = K_UNITS[unit]

        @pl.when(needed[blk])
        def _():
            for h in range(h0, h0 + n):
                score_other(blk, h)

    loads[0].wait()
    split_heads(k_raw, num_kv, put_k)
    pl.when(low)(lambda: pl.semaphore_wait(barrier, 3))
    pl.when(top)(lambda: pl.semaphore_wait(barrier, 2))
    own_x(0)
    own_y(1)
    own_x(1)
    own_y(0)
    own_partner(range(NK))
    loads[1].wait()
    split_heads(v_raw, num_kv, put_v)
    own_values(True)
    loads[2].wait()
    split_heads(q_raw, num_heads, put_q)
    arrive(None, range(NK), [PT])
    for h in range(num_kv):
        score_own(h)

    arrive_x(0)
    relay([0], X)
    arrive(top, [1], [Y])
    relay([1], Y)
    share([0], X)
    share([1], Y)
    own_values(False)
    own_partner(range(NK, NK + NV))
    arrive(right, [0], [PX])
    scores_of(X, 0)
    arrive(top, [1], [PY])
    scores_of(Y, 1)
    arrive_x(1)
    share([1], X)
    arrive(top, [0], [Y])
    share([0], Y)
    arrive(right, [1], [PX])
    scores_of(X, 1)
    arrive(top, [0], [PY])
    scores_of(Y, 0)
    log2_scale = dim ** -0.5 * math.log2(math.e)
    step_rows = 64

    def row_max(h):
        mp[h] = jnp.broadcast_to(jnp.max(mp[h], axis=-1, keepdims=True) * log2_scale, (rows, tokens))

    def probs(h, blocks):
        for r0 in range(0, rows, step_rows):
            r = pl.ds(r0, step_rows)
            m = mp[h, r, :]
            total = None
            for blk in blocks:
                for c0 in (0, tokens):
                    p = jnp.exp2(s_buf[blk, h, r, pl.ds(c0, tokens)] * log2_scale - m)
                    p_buf[blk, h, r, pl.ds(c0, tokens)] = p.astype(BF16)
                    total = p if total is None else total + p
            lsum[h, r, :] = total

    def row_sum(h):
        lsum[h] = jnp.broadcast_to(1.0 / jnp.sum(lsum[h], axis=-1, keepdims=True), (rows, dim))

    def far_scores(h):
        s = scores(Z, h)
        s_buf[Z, h] = s
        mz[h] = jnp.maximum(s[:, :tokens], s[:, tokens:])

    def far_probs(h):
        for r0 in range(0, rows, step_rows):
            r = pl.ds(r0, step_rows)
            old = mp[h, r, :]
            m = jnp.maximum(old, jnp.broadcast_to(jnp.max(mz[h, r, :], axis=-1, keepdims=True) * log2_scale, (step_rows, tokens)))
            factor = jnp.exp2(old - m)
            mp[h, r, :] = factor
            total = lsum[h, r, :] * factor
            for c0 in (0, tokens):
                p = jnp.exp2(s_buf[Z, h, r, pl.ds(c0, tokens)] * log2_scale - m)
                p_buf[Z, h, r, pl.ds(c0, tokens)] = p.astype(BF16)
                total = total + p
            lsum[h, r, :] = total

    def weighted(h, blocks):
        total = None
        for blk in blocks:
            vv = vbuf[h, pl.ds(pl.multiple_of(chip_of[blk] * pair, pair), pair), :]
            part = lax.dot_general(p_buf[blk, h], vv, (((1,), (0,)), ((), ())), preferred_element_type=F32)
            total = part if total is None else total + part
        return total

    def near(h, blocks):
        acc[h] = weighted(h, [blk for blk in blocks if blk != Z])

    def last(h, blocks):
        out = acc[h] if Z not in blocks else acc[h] * mp[h] + weighted(h, [Z])
        out = out * lsum[h]
        for n in range(group):
            f_buf[pl.ds(h * group + n, tokens, stride=num_heads), :] = out[n * tokens : (n + 1) * tokens, :]

    def values_from_links(u):
        h0, n, way = V_UNITS[u]
        second = [NK + NV + h for h in range(h0, h0 + n)]
        arrive(top, [NK + u], [Y])
        if way == 1:
            relay(second, Y)
        share([NK + u], Y)
        arrive_x(NK + u)
        if way == 0:
            relay(second, X)
        share([NK + u], X)

    def values_from_partner(u):
        arrive(None, [NK + u], [PT])
        arrive(right, [NK + u], [PX])
        arrive(top, [NK + u], [PY])

    def stage(heads):
        def body(blocks):
            for h in heads:
                if h == 0:
                    row_max(0)
                if h + 1 < num_kv:
                    row_max(h + 1)
                probs(h, [blk for blk in blocks if blk != Z])

        by_role(body)

    def far_stage(heads):
        def body(blocks):
            for h in heads:
                if Z in blocks:
                    if h == 0:
                        far_scores(0)
                    if h + 1 < num_kv:
                        far_scores(h + 1)
                    if h < num_kv:
                        far_probs(h)
                if h > 0:
                    row_sum(h - 1)

        by_role(body)

    def second_hop(heads):
        for h in heads:
            arrive(top, [NK + NV + h], [Z])
            share([NK + NV + h], Z)

    def last_stage(heads):
        arrive(top, [NK + NV + h for h in heads], [PZ])

        def body(blocks):
            for h in heads:
                last(h, blocks)

        by_role(body)

    def near_stage(u):
        h0, n, _ = V_UNITS[u]

        def body(blocks):
            for h in range(h0, h0 + n):
                near(h, blocks)

        by_role(body)

    stage((0, 1))
    for u in range(NK):
        arrive(top, [u], [Z])
        share([u], Z)
    stage((2, 3))
    stage((4, 5))
    stage((6, 7))
    arrive(top, range(NK), [PZ])
    turn = (1, 3, 0, 2)
    for i, u in enumerate(turn):
        values_from_links(u)
        far_stage((2 * i, 2 * i + 1) if i < NV - 1 else (2 * i, 2 * i + 1, num_kv))
        if i > 0:
            values_from_partner(turn[i - 1])
            near_stage(turn[i - 1])
    second_hop((0, 2))
    second_hop((1, 3))
    values_from_partner(turn[-1])
    near_stage(turn[-1])
    second_hop((4, 6))
    last_stage((0, 2))
    second_hop((5, 7))
    last_stage((1, 3))
    last_stage((4, 6))
    last_stage((5, 7))

    def narrow(i, carry):
        t = pl.multiple_of(i * 16, 16)
        o_ref[pl.ds(t, 16)] = f_buf[pl.ds(pl.multiple_of(t * num_heads, 16 * num_heads), 16 * num_heads), :].reshape(16, num_heads, dim).astype(BF16)
        return carry

    lax.fori_loop(0, tokens // 16, narrow, 0)
    for cond, copies in drains:
        when(cond, lambda: [copy.wait_send() for copy in copies] and None)


def solution(mesh):
    seq_spec = P(("batch", "cx", "cy"), None, None)
    ranks = mesh.shape["cx"] * mesh.shape["cy"]

    def local(q, k, v):
        tokens, heads, dim = q.shape
        kv = k.shape[1]
        rows = heads // kv * tokens
        hbm = pl.BlockSpec(memory_space=pltpu.HBM)
        return pl.pallas_call(
            kernel,
            out_shape=pltpu.VMEM(q.shape, q.dtype),
            in_specs=[hbm, hbm, hbm],
            out_specs=pl.BlockSpec(memory_space=pltpu.VMEM),
            scratch_shapes=[
                pltpu.VMEM((kv, ranks * tokens, dim), BF16),
                pltpu.VMEM((kv, ranks * tokens, dim), BF16),
                pltpu.VMEM((kv, rows, dim), BF16),
                pltpu.VMEM((4, kv, rows, 2 * tokens), F32),
                pltpu.VMEM((4, kv, rows, 2 * tokens), BF16),
                pltpu.VMEM((kv, rows, dim), F32),
                pltpu.VMEM((kv, rows, dim), F32),
                pltpu.VMEM((kv, rows, dim), F32),
                pltpu.VMEM((kv, rows, dim), F32),
                pltpu.VMEM((tokens, heads, dim), BF16),
                pltpu.VMEM((tokens, kv, dim), BF16),
                pltpu.VMEM((tokens, kv, dim), BF16),
                pltpu.VMEM((tokens * heads, dim), F32),
                pltpu.SemaphoreType.DMA((3,)),
                pltpu.SemaphoreType.DMA((80,)),
                pltpu.SemaphoreType.DMA((7 * NU,)),
            ],
            compiler_params=pltpu.CompilerParams(collective_id=0, has_side_effects=True, vmem_limit_bytes=57 * 2**20),
        )(*[pltpu.with_memory_space_constraint(a, pltpu.HBM) for a in (q, k, v)])

    return jax.shard_map(local, mesh=mesh, in_specs=(seq_spec, seq_spec, seq_spec), out_specs=seq_spec, check_vma=False)
```

```python
import math

import jax
import jax.numpy as jnp
from jax import lax
from jax.experimental import pallas as pl
from jax.experimental.pallas import tpu as pltpu
from jax.sharding import PartitionSpec as P

MESH = pl.DeviceIdType.MESH
F32 = jnp.float32
BF16 = jnp.bfloat16

K_UNITS = ((0, 4, 0), (4, 4, 1))
V_UNITS = ((0, 2, 0), (2, 2, 1), (4, 2, 0), (6, 2, 1))
W_UNITS = tuple((h, 1, (h // 2) % 2) for h in range(8))
NK, NV, NW = len(K_UNITS), len(V_UNITS), len(W_UNITS)
UNITS = K_UNITS + V_UNITS + W_UNITS
NU = len(UNITS)
X, Y, Z, OWN = range(4)
PT, PX, PY, PZ = 3, 4, 5, 6
ME = 7
ROLE_BLOCKS = ((OWN,), (OWN, X), (OWN, Y, Z), (OWN, X, Y, Z))


def kernel(q_hbm, k_hbm, v_hbm, o_ref, kbuf, vbuf, qt, s_buf, p_buf, mp, mz, lsum, acc, q_raw, k_raw, v_raw, f_buf, lsem, ssem, rsem):
    tokens, num_heads, dim = q_hbm.shape
    num_kv = k_hbm.shape[1]
    group = num_heads // num_kv
    rows = group * tokens
    pair = 2 * tokens
    iy, cy = lax.axis_index("cx"), lax.axis_index("cy")
    ix, core = cy // 2, cy % 2
    chip = iy * 2 + ix
    cy_x = (cy + 2) % 4
    cy_p = cy + 1 - 2 * core
    cy_xp = (cy_p + 2) % 4
    iy_o = 1 - iy
    rank_of = {ME: iy * 4 + cy, X: iy * 4 + cy_x, Y: iy_o * 4 + cy, Z: iy_o * 4 + cy_x, PT: iy * 4 + cy_p, PX: iy * 4 + cy_xp, PY: iy_o * 4 + cy_p, PZ: iy_o * 4 + cy_xp}
    dev_x, dev_y, dev_p = (0, iy, cy_x), (0, iy_o, cy), (0, iy, cy_p)
    chip_of = {X: iy * 2 + 1 - ix, Y: iy_o * 2 + ix, Z: iy_o * 2 + 1 - ix, OWN: chip}

    loads = [pltpu.make_async_copy(k_hbm, k_raw, lsem.at[0]), pltpu.make_async_copy(v_hbm, v_raw, lsem.at[1]), pltpu.make_async_copy(q_hbm, q_raw, lsem.at[2])]
    for load in loads:
        load.start()
    barrier = pltpu.get_barrier_semaphore()
    pl.semaphore_signal(barrier, inc=1, device_id=dev_p, device_id_type=MESH)
    pl.semaphore_signal(barrier, inc=1, device_id=dev_x, device_id_type=MESH)

    @pl.when(iy == 1)
    def _():
        pl.semaphore_signal(barrier, inc=1, device_id=dev_y, device_id_type=MESH)


    def split_heads(raw, heads, put):
        step = 32

        def widen(i, carry):
            t = pl.multiple_of(i * step, step)
            f_buf[pl.ds(pl.multiple_of(t * heads, step * heads), step * heads), :] = raw[pl.ds(t, step)].astype(F32).reshape(step * heads, dim)
            return carry

        lax.fori_loop(0, tokens // step, widen, 0)
        for h in range(heads):
            put(h, f_buf[pl.ds(h, tokens, stride=heads), :].astype(BF16))

    my_rows = pl.ds(pl.multiple_of(rank_of[ME] * tokens, tokens), tokens)

    def put_k(h, val):
        kbuf[h, my_rows, :] = val

    def put_v(h, val):
        vbuf[h, my_rows, :] = val

    def put_q(h, val):
        qt[h // group, pl.ds((h % group) * tokens, tokens), :] = val

    top, low, right, left = iy == 1, iy == 0, ix == 1, ix == 0
    not_third, not_last = chip != 2, chip != 3
    sends = []

    def when(cond, body):
        body() if cond is None else pl.when(cond)(body)

    def piece(unit, src):
        h0, n, _ = UNITS[unit]
        buf = kbuf if unit < NK else vbuf
        return buf.at[pl.ds(h0, n), pl.ds(pl.multiple_of(rank_of[src] * tokens, tokens), tokens), :]

    def send(cond, moves):
        first = len(sends)
        for i, (unit, src, dev, as_src) in enumerate(moves):
            ref = piece(unit, src)
            sends.append(pltpu.make_async_remote_copy(ref, ref, ssem.at[first + i], rsem.at[as_src * NU + unit], device_id=dev, device_id_type=MESH))
        copies = sends[first:]
        when(cond, lambda: [copy.start() for copy in copies] and None)
        drains.append((cond, copies))

    drains = []

    def arrive(cond, units, srcs):
        def body():
            for unit in units:
                for src in srcs:
                    ref = piece(unit, src)
                    pltpu.make_async_remote_copy(ref, ref, ssem.at[0], rsem.at[src * NU + unit], device_id=dev_p, device_id_type=MESH).wait_recv()

        when(cond, body)

    def path(unit):
        return UNITS[unit][2]

    def own_x(unit):
        send(left if path(unit) else not_last, [(unit, ME, dev_x, X)])

    def own_y(unit):
        send(low, [(unit, ME, dev_y, Y)])

    def own_values(first):
        if first:
            for u in (0, 2, 1, 3):
                send(chip == 0, [(NK + u, ME, dev_x, X)])
            return
        for a, b in ((1, 1), (3, 3), (0, 0), (2, 2)):
            send(chip == 2 if path(NK + a) else (chip + 1) // 2 == 1, [(NK + a, ME, dev_x, X)])
            send(low, [(NK + b, ME, dev_y, Y)])

    def own_partner(units):
        send(None, [(unit, ME, dev_p, PT) for unit in units])

    def arrive_x(unit):
        arrive(right if path(unit) else not_third, [unit], [X])

    def share(units, src):
        send(right if src == X else top, [(unit, src, dev_p, {X: PX, Y: PY, Z: PZ}[src]) for unit in units])

    def relay(units, src):
        send({X: low, Y: top}[src], [(unit, src, {X: dev_y, Y: dev_x}[src], Z) for unit in units])

    def by_role(body):
        for role, blocks in enumerate(ROLE_BLOCKS):
            @pl.when(chip == role)
            def _():
                body(blocks)

    def scores(blk, h):
        kk = kbuf[h, pl.ds(pl.multiple_of(chip_of[blk] * pair, pair), pair), :]
        return lax.dot_general(qt[h], kk, (((1,), (1,)), ((), ())), preferred_element_type=F32)

    def score_own(h):
        s = scores(OWN, h)
        q_pos = lax.broadcasted_iota(jnp.int32, (rows, pair), 0) % tokens + core * tokens
        k_pos = lax.broadcasted_iota(jnp.int32, (rows, pair), 1)
        s = jnp.where(k_pos <= q_pos, s, -jnp.inf)
        s_buf[OWN, h] = s
        mp[h] = jnp.maximum(s[:, :tokens], s[:, tokens:])

    def score_other(blk, h):
        s = scores(blk, h)
        s_buf[blk, h] = s
        mp[h] = jnp.maximum(mp[h], jnp.maximum(s[:, :tokens], s[:, tokens:]))

    needed = {X: ix == 1, Y: iy == 1}

    def scores_of(blk, unit):
        h0, n, _ = K_UNITS[unit]

        @pl.when(needed[blk])
        def _():
            for h in range(h0, h0 + n):
                score_other(blk, h)

    loads[0].wait()
    split_heads(k_raw, num_kv, put_k)
    pl.when(low)(lambda: pl.semaphore_wait(barrier, 3))
    pl.when(top)(lambda: pl.semaphore_wait(barrier, 2))
    own_x(0)
    own_y(1)
    own_x(1)
    own_y(0)
    own_partner(range(NK))
    loads[1].wait()
    split_heads(v_raw, num_kv, put_v)
    own_values(True)
    loads[2].wait()
    split_heads(q_raw, num_heads, put_q)
    arrive(None, range(NK), [PT])
    for h in range(num_kv):
        score_own(h)

    arrive_x(0)
    relay([0], X)
    arrive(top, [1], [Y])
    relay([1], Y)
    share([0], X)
    share([1], Y)
    own_values(False)
    own_partner(range(NK, NK + NV))
    arrive(right, [0], [PX])
    scores_of(X, 0)
    arrive(top, [1], [PY])
    scores_of(Y, 1)
    arrive_x(1)
    share([1], X)
    arrive(top, [0], [Y])
    share([0], Y)
    arrive(right, [1], [PX])
    scores_of(X, 1)
    arrive(top, [0], [PY])
    scores_of(Y, 0)
    log2_scale = dim ** -0.5 * math.log2(math.e)
    step_rows = 64

    def row_max(h):
        mp[h] = jnp.broadcast_to(jnp.max(mp[h], axis=-1, keepdims=True) * log2_scale, (rows, tokens))

    def probs(h, blocks):
        for r0 in range(0, rows, step_rows):
            r = pl.ds(r0, step_rows)
            m = mp[h, r, :]
            total = None
            for blk in blocks:
                for c0 in (0, tokens):
                    p = jnp.exp2(s_buf[blk, h, r, pl.ds(c0, tokens)] * log2_scale - m)
                    p_buf[blk, h, r, pl.ds(c0, tokens)] = p.astype(BF16)
                    total = p if total is None else total + p
            lsum[h, r, :] = total

    def row_sum(h):
        lsum[h] = jnp.broadcast_to(1.0 / jnp.sum(lsum[h], axis=-1, keepdims=True), (rows, dim))

    def far_scores(h):
        s = scores(Z, h)
        s_buf[Z, h] = s
        mz[h] = jnp.maximum(s[:, :tokens], s[:, tokens:])

    def far_probs(h):
        for r0 in range(0, rows, step_rows):
            r = pl.ds(r0, step_rows)
            old = mp[h, r, :]
            m = jnp.maximum(old, jnp.broadcast_to(jnp.max(mz[h, r, :], axis=-1, keepdims=True) * log2_scale, (step_rows, tokens)))
            factor = jnp.exp2(old - m)
            mp[h, r, :] = factor
            total = lsum[h, r, :] * factor
            for c0 in (0, tokens):
                p = jnp.exp2(s_buf[Z, h, r, pl.ds(c0, tokens)] * log2_scale - m)
                p_buf[Z, h, r, pl.ds(c0, tokens)] = p.astype(BF16)
                total = total + p
            lsum[h, r, :] = total

    def weighted(h, blocks):
        total = None
        for blk in blocks:
            vv = vbuf[h, pl.ds(pl.multiple_of(chip_of[blk] * pair, pair), pair), :]
            part = lax.dot_general(p_buf[blk, h], vv, (((1,), (0,)), ((), ())), preferred_element_type=F32)
            total = part if total is None else total + part
        return total

    def near(h, blocks):
        acc[h] = weighted(h, [blk for blk in blocks if blk != Z])

    def last(h, blocks):
        out = acc[h] if Z not in blocks else acc[h] * mp[h] + weighted(h, [Z])
        out = out * lsum[h]
        for n in range(group):
            f_buf[pl.ds(h * group + n, tokens, stride=num_heads), :] = out[n * tokens : (n + 1) * tokens, :]

    def values_from_links(u):
        h0, n, way = V_UNITS[u]
        second = [NK + NV + h for h in range(h0, h0 + n)]
        arrive(top, [NK + u], [Y])
        if way == 1:
            relay(second, Y)
        share([NK + u], Y)
        arrive_x(NK + u)
        if way == 0:
            relay(second, X)
        share([NK + u], X)

    def values_from_partner(u):
        arrive(None, [NK + u], [PT])
        arrive(right, [NK + u], [PX])
        arrive(top, [NK + u], [PY])

    def stage(heads):
        def body(blocks):
            for h in heads:
                if h == 0:
                    row_max(0)
                if h + 1 < num_kv:
                    row_max(h + 1)
                probs(h, [blk for blk in blocks if blk != Z])

        by_role(body)

    def far_stage(heads):
        def body(blocks):
            for h in heads:
                if Z in blocks:
                    if h == 0:
                        far_scores(0)
                    if h + 1 < num_kv:
                        far_scores(h + 1)
                    if h < num_kv:
                        far_probs(h)
                if h > 0:
                    row_sum(h - 1)

        by_role(body)

    def second_hop(heads):
        for h in heads:
            arrive(top, [NK + NV + h], [Z])
            share([NK + NV + h], Z)

    def last_stage(heads):
        arrive(top, [NK + NV + h for h in heads], [PZ])

        def body(blocks):
            for h in heads:
                last(h, blocks)

        by_role(body)

    def near_stage(u):
        h0, n, _ = V_UNITS[u]

        def body(blocks):
            for h in range(h0, h0 + n):
                near(h, blocks)

        by_role(body)

    stage((0, 1))
    for u in range(NK):
        arrive(top, [u], [Z])
        share([u], Z)
    stage((2, 3))
    stage((4, 5))
    stage((6, 7))
    arrive(top, range(NK), [PZ])
    turn = (1, 3, 0, 2)
    for i, u in enumerate(turn):
        values_from_links(u)
        far_stage((2 * i, 2 * i + 1) if i < NV - 1 else (2 * i, 2 * i + 1, num_kv))
        if i > 0:
            values_from_partner(turn[i - 1])
            near_stage(turn[i - 1])
    second_hop((0, 2))
    second_hop((1, 3))
    values_from_partner(turn[-1])
    second_hop((4, 6))
    near_stage(turn[-1])
    second_hop((5, 7))
    last_stage((0, 2, 1, 3))
    last_stage((4, 6))
    last_stage((5, 7))

    def narrow(i, carry):
        t = pl.multiple_of(i * 16, 16)
        o_ref[pl.ds(t, 16)] = f_buf[pl.ds(pl.multiple_of(t * num_heads, 16 * num_heads), 16 * num_heads), :].reshape(16, num_heads, dim).astype(BF16)
        return carry

    lax.fori_loop(0, tokens // 16, narrow, 0)
    for cond, copies in drains:
        when(cond, lambda: [copy.wait_send() for copy in copies] and None)


def solution(mesh):
    seq_spec = P(("batch", "cx", "cy"), None, None)
    ranks = mesh.shape["cx"] * mesh.shape["cy"]

    def local(q, k, v):
        tokens, heads, dim = q.shape
        kv = k.shape[1]
        rows = heads // kv * tokens
        hbm = pl.BlockSpec(memory_space=pltpu.HBM)
        return pl.pallas_call(
            kernel,
            out_shape=pltpu.VMEM(q.shape, q.dtype),
            in_specs=[hbm, hbm, hbm],
            out_specs=pl.BlockSpec(memory_space=pltpu.VMEM),
            scratch_shapes=[
                pltpu.VMEM((kv, ranks * tokens, dim), BF16),
                pltpu.VMEM((kv, ranks * tokens, dim), BF16),
                pltpu.VMEM((kv, rows, dim), BF16),
                pltpu.VMEM((4, kv, rows, 2 * tokens), F32),
                pltpu.VMEM((4, kv, rows, 2 * tokens), BF16),
                pltpu.VMEM((kv, rows, dim), F32),
                pltpu.VMEM((kv, rows, dim), F32),
                pltpu.VMEM((kv, rows, dim), F32),
                pltpu.VMEM((kv, rows, dim), F32),
                pltpu.VMEM((tokens, heads, dim), BF16),
                pltpu.VMEM((tokens, kv, dim), BF16),
                pltpu.VMEM((tokens, kv, dim), BF16),
                pltpu.VMEM((tokens * heads, dim), F32),
                pltpu.SemaphoreType.DMA((3,)),
                pltpu.SemaphoreType.DMA((80,)),
                pltpu.SemaphoreType.DMA((7 * NU,)),
            ],
            compiler_params=pltpu.CompilerParams(collective_id=0, has_side_effects=True, vmem_limit_bytes=57 * 2**20),
        )(*[pltpu.with_memory_space_constraint(a, pltpu.HBM) for a in (q, k, v)])

    return jax.shard_map(local, mesh=mesh, in_specs=(seq_spec, seq_spec, seq_spec), out_specs=seq_spec, check_vma=False)
```
